32 devices in a mesh: member: 4 (over y, x), space: 8 (over z, core).
Axes of the slice: x: 2, y: 2, z: 4, core: 2. Of those that a mesh axis runs over, the one named last changes fastest.
Arguments:
- hidden_codes: bfloat16 [8, 256, 23040], P('member', None, 'space'), may hold values from -6 to 6
- w_in: bfloat16 [1024, 256], replicated, may hold values from -0.375 to 0.375
- b_in: float32 [1024], replicated, may hold values from -3 to 3
- w_out: bfloat16 [72, 1024], replicated, may hold values from -0.1875 to 0.1875
- b_out: float32 [72], replicated, may hold values from -3 to 3
- target: bfloat16 [72, 23040], P(None, 'space'), may hold values from -6 to 6
- band_start: int32 [8], P('space'), may hold values from 0 to 14, as said below
Outputs:
- code_sensitivity: bfloat16 [8, 256, 23040], P('member', None, 'space')
- grad_w_in: float32 [1024, 256], replicated
- grad_w_out: float32 [72, 1024], replicated
- grad_b_in: float32 [1024], replicated
The draws below stay inside these ranges and needn't reach their ends.
Inputs may be any that keep to these rules, and one draw needn't show every extreme that they name: band_start holds each of 0, 2, 4, ... once, in some order.
All inputs are finite; a program needn't handle non-finite values.
Results may differ from the reference program's by a relative error of at most 0.005.
The reference program's roundings to bfloat16 on the way count: a program that leaves them out, or rounds other values in their place, can miss the bound.
Values may be sent and summed in bfloat16 or wider, within the bound.
A program may use at most 128 MiB of HBM per device.

```python
import math
import jax
import jax.numpy as jnp
from jax import lax

CHANNELS = 72
HID = 1024
LATENT = 256
LON = 1440
ROWS_DEV = 2
MEMBERS = 8
CELLS = 23040
N_SPACE = 8


def draw_band_start(key, part):
    order = jax.random.permutation(jax.random.fold_in(key, 11), N_SPACE)
    return (order * ROWS_DEV).astype(jnp.int32)


def level_of(rng, dims, cuts, smallest, high):
    def one(dim, parts):
        heights = jax.random.uniform(jax.random.fold_in(jax.random.fold_in(rng, 6), dim), (parts,), jnp.float32, smallest / len(cuts), high / len(cuts))
        return jnp.repeat(jnp.exp(heights), dims[dim] // parts).reshape((-1,) + (1,) * (len(dims) - dim - 1))

    level = one(*cuts[0])
    for cut in cuts[1:]:
        level = level * one(*cut)
    return level


def bell_draw(rng, dims, scale, reach, split=(), kind=jnp.bfloat16):
    factor_of = level_of(rng, dims, split, -0.22, 0.18) if split else 1.0
    values = jax.random.normal(rng, dims, jnp.float32) * scale * factor_of
    return jnp.minimum(jnp.maximum(values, -reach), reach).astype(kind)


def setup_inputs(seed: int = 0) -> dict:
    key_list = jax.random.split(jax.random.key(seed), 8)
    hidden_codes = bell_draw(key_list[0], (MEMBERS, LATENT, CELLS), 1.0, 6.0, ((0, 4), (2, 8)))
    w_in = bell_draw(key_list[1], (HID, LATENT), LATENT ** -0.5, 0.375)
    b_in = bell_draw(key_list[2], (HID,), 0.5, 3.0, (), jnp.float32)
    w_out = bell_draw(key_list[3], (CHANNELS, HID), HID ** -0.5, 0.1875)
    b_out = bell_draw(key_list[4], (CHANNELS,), 0.5, 3.0, (), jnp.float32)
    target = bell_draw(key_list[5], (CHANNELS, CELLS), 1.0, 6.0, ((1, 8),))
    band_start = draw_band_start(jax.random.fold_in(key_list[7], 71), 0)
    return dict(hidden_codes=hidden_codes, w_in=w_in, b_in=b_in, w_out=w_out, b_out=b_out, target=target, band_start=band_start)


def slope(diff):
    return diff / jnp.sqrt(diff * diff + 0.0625)

def area_weights(band_start):
    rows = band_start[:, None] + jnp.arange(ROWS_DEV, dtype=jnp.int32)[None, :]
    angle = (rows.astype(jnp.float32) + 0.5) * (math.pi / (ROWS_DEV * N_SPACE)) - math.pi / 2
    return jnp.repeat(jnp.cos(angle).reshape(-1), LON)

def reference(hidden_codes, w_in, b_in, w_out, b_out, target, band_start):
    area = area_weights(band_start)
    members = hidden_codes.shape[0]
    cells = hidden_codes.shape[2]

    def apply_readout(inputs):
        pre = jnp.dot(w_in, inputs, preferred_element_type=jnp.float32) + b_in[:, None]
        act = jax.nn.gelu(pre).astype(jnp.bfloat16)
        return (jnp.dot(w_out, act, preferred_element_type=jnp.float32) + b_out[:, None]).astype(jnp.bfloat16)
    predicted_maps = lax.map(apply_readout, hidden_codes)
    goal = target.astype(jnp.float32)

    def cross_sensitivity(mine):
        diagonal_contribution = mine.astype(jnp.float32)

        def lone_realization(total, other):
            return (total + slope(diagonal_contribution - other.astype(jnp.float32)), None)
        couple_index, discarded_value = lax.scan(lone_realization, jnp.zeros_like(diagonal_contribution), predicted_maps)
        return (area[None, :] * (slope(diagonal_contribution - goal) - couple_index / members)).astype(jnp.bfloat16)
    prediction_sensitivity = lax.map(cross_sensitivity, predicted_maps)

    def reverse_sweep(carry, items):
        inputs, prediction_adjoint = items
        pre = jnp.dot(w_in, inputs, preferred_element_type=jnp.float32) + b_in[:, None]
        act_f, undo = jax.vjp(jax.nn.gelu, pre)
        act = act_f.astype(jnp.bfloat16)
        dact = jnp.dot(w_out.T, prediction_adjoint, preferred_element_type=jnp.float32)
        dpre = undo(dact)[0].astype(jnp.bfloat16)
        dlat = jnp.dot(w_in.T, dpre, preferred_element_type=jnp.float32).astype(jnp.bfloat16)
        adjoint_entry_matrix = carry[0] + jnp.dot(dpre, inputs.T, preferred_element_type=jnp.float32)
        adjoint_exit_matrix = carry[1] + jnp.dot(prediction_adjoint, act.T, preferred_element_type=jnp.float32)
        adjoint_offset = carry[2] + lax.optimization_barrier(jnp.sum(dpre.astype(jnp.float32), axis=1))
        return ((adjoint_entry_matrix, adjoint_exit_matrix, adjoint_offset), dlat)
    opening_offset = (jnp.zeros(w_in.shape, jnp.float32), jnp.zeros(w_out.shape, jnp.float32), jnp.zeros(b_in.shape, jnp.float32))
    (adjoint_entry_matrix, adjoint_exit_matrix, adjoint_offset), code_sensitivity = lax.scan(reverse_sweep, opening_offset, (hidden_codes, prediction_sensitivity))
    scale = 1.0 / math.sqrt(members * (cells // N_SPACE))
    return (code_sensitivity, adjoint_entry_matrix * scale, adjoint_exit_matrix * scale, adjoint_offset * scale)
```

```python
import functools
import math

import jax
import jax.numpy as jnp
from jax import lax
from jax.experimental import pallas as pl
from jax.experimental.pallas import tpu as pltpu
from jax.sharding import PartitionSpec as P

LON = 1440
BR = 256
MESH = pl.DeviceIdType.MESH
NT = (((1,), (1,)), ((), ()))
F32 = jnp.float32
BF16 = jnp.bfloat16
K0 = math.sqrt(2.0 / math.pi)
K1 = K0 * 0.044715


def slope(diff):
    return diff * lax.rsqrt(diff * diff + 0.0625)


def gelu_slope(h):
    q = h * h
    t = jnp.tanh(h * (2.0 * K0 + (8.0 * K1) * q))
    v = (1.0 - t) * (h * (2.0 * K0 + (24.0 * K1) * q))
    return (1.0 + t) * (1.0 + v)


def kernel(
    msize,
    ssize,
    cells,
    hid_ref,
    w_in_ref,
    b_in_ref,
    w_out_ref,
    b_out_ref,
    tgt_ref,
    start_ref,
    code_ref,
    gwi_ref,
    gwo_ref,
    gb_ref,
    tgt,
    area,
    act,
    pre,
    fcs,
    fcr,
    dfr,
    acc_i,
    acc_o,
    acc_b,
    half,
    r1,
    s2,
    r2,
    r3,
    full,
    x1s,
    x1r,
    x2s,
    x2r,
    p1s,
    p1r,
    p2s,
    p2r,
    p3s,
    p3r,
    p4s,
    p4r,
    p5s,
    p5r,
    w_half,
    w_in_t,
    w_out_t,
    b_in,
    b_out,
    load,
):
    local = hid_ref.shape[0]
    hidden = w_in_ref.shape[0]
    latent = w_in_ref.shape[1]
    chans = w_out_ref.shape[0]
    width = tgt.shape[2]
    dfs = fcs
    members = local * msize
    zsize = ssize // 2
    ysize = msize // 2
    nb = hidden // BR
    hr = BR // 2
    pr = hr // msize
    parts = x2s.shape[1]
    me = lax.axis_index("member")
    sp = lax.axis_index("space")
    core = lax.rem(sp, 2)
    z = sp // 2
    partner = z * 2 + (1 - core)
    mx = lax.rem(me, 2)
    my = me // 2

    def mpeer(k):
        return lax.rem(my + k // 2, ysize) * 2 + lax.rem(mx + k, 2)

    def mfrom(k):
        return lax.rem(my + ysize - k // 2, ysize) * 2 + lax.rem(mx + k, 2)

    def zpeer(k):
        return lax.rem(z + k, zsize) * 2 + core

    barrier = pltpu.get_barrier_semaphore()
    pl.semaphore_signal(barrier, inc=1, device_id=(me, partner), device_id_type=MESH)
    for k in range(1, msize):
        pl.semaphore_signal(barrier, inc=1, device_id=(mpeer(k), sp), device_id_type=MESH)
    for k in range(1, zsize):
        pl.semaphore_signal(barrier, inc=1, device_id=(me, zpeer(k)), device_id_type=MESH)

    last = msize - 1
    rest = cells - last * width

    def span(c):
        return width if c < last else rest

    def fetch(c, m, n, lo):
        return pltpu.make_async_copy(
            hid_ref.at[m, pl.ds(lo, n)], code_ref.at[m, pl.ds(lo, n)], load.at[c, m]
        )

    def codes(c, m):
        return code_ref[m, pl.ds(pl.multiple_of(c * width, width), width), :]

    for k in range(msize - 1, -1, -1):
        first = mpeer(k)

        @pl.when(first < last)
        def _():
            for m in range(local):
                fetch(first, m, width, pl.multiple_of(first * width, width)).start()

        @pl.when(first == last)
        def _():
            for m in range(local):
                fetch(last, m, rest, last * width).start()

    if rest < width:
        code_ref[:, cells:, :] = jnp.zeros((local, width - rest, latent), BF16)
        tgt[last] = jnp.zeros(tgt.shape[1:], BF16)
    b_in[...] = jnp.transpose(jnp.broadcast_to(b_in_ref[...] * 0.5, (128, hidden)))
    b_out[...] = jnp.transpose(jnp.broadcast_to(b_out_ref[...], (128, chans)))
    w_half[...] = w_in_ref[...] * 0.5

    def x1(k, m):
        return pltpu.make_async_remote_copy(
            src_ref=fcs.at[mpeer(k), m],
            dst_ref=fcr.at[me, m],
            send_sem=x1s.at[k, m],
            recv_sem=x1r.at[k, m],
            device_id=(mpeer(k), sp),
            device_id_type=MESH,
        )

    share_lanes = width // parts

    def x2(k, p):
        lanes = pl.ds(p * share_lanes, share_lanes)
        return pltpu.make_async_remote_copy(
            src_ref=dfs.at[mpeer(k), :, :, lanes],
            dst_ref=dfr.at[me, :, :, lanes],
            send_sem=x2s.at[k, p],
            recv_sem=x2r.at[k, p],
            device_id=(mpeer(k), sp),
            device_id_type=MESH,
        )

    def ready(c):
        for m in range(local):

            @pl.when(c < last)
            def _():
                fetch(c, m, width, 0).wait()

            @pl.when(c == last)
            def _():
                fetch(c, m, rest, 0).wait()

    def forward(c, m):
        x = lax.dot_general(w_half[...], codes(c, m), NT, preferred_element_type=F32)
        h = x + b_in[:, :1]
        pre[c, m] = h
        t = jnp.tanh(h * (2.0 * K0 + (8.0 * K1) * (h * h)))
        act[c, m] = (h + h * t).astype(BF16)
        fc = jnp.dot(w_out_ref[...], act[c, m], preferred_element_type=F32)
        fcs[c, m] = (fc + b_out[:, :1]).astype(BF16)

    def step(i, carry):
        k = msize - 1 - i
        c = mpeer(k)
        with jax.named_scope("fwd"):
            ready(c)
            for m in range(local):
                forward(c, m)

            @pl.when(i == 0)
            def _():
                pl.semaphore_wait(barrier, msize + zsize - 1)

            for m in range(local):
                x1(k, m).start()
        return carry

    lax.fori_loop(0, msize - 1, step, 0)
    with jax.named_scope("fwdme"):
        ready(me)
        for m in range(local):
            forward(me, m)
    fcr[me] = fcs[me]

    def slopes(c, m):
        def block(i, carry):
            rows = pl.ds(pl.multiple_of(i * 128, 128), 128)
            pre[c, m, rows, :] = gelu_slope(pre[c, m, rows, :])
            return carry

        lax.fori_loop(0, hidden // 128, block, 0)

    work = [(k, m) for k in range(msize - 1) for m in range(local)]
    early = 3

    with jax.named_scope("gap1"):
        place = me * width + lax.broadcasted_iota(jnp.int32, (1, width), 1)
        row = jnp.zeros((1, width), jnp.int32) + start_ref[0]
        for r in range(1, cells // LON):
            row = row + jnp.where(place >= r * LON, 1, 0)
        angle = (row.astype(F32) + 0.5) * (math.pi / (cells // LON * ssize)) - math.pi / 2
        area[...] = jnp.where(place < cells, jnp.cos(angle), 0.0)
        acc_i[...] = jnp.zeros_like(acc_i)
        acc_o[...] = jnp.zeros_like(acc_o)
        acc_b[...] = jnp.zeros_like(acc_b)
        for c in range(msize):
            n = span(c)
            tgt[c, :, :n] = tgt_ref[:, c * width : c * width + n]
        w_in_t[...] = jnp.transpose(w_in_ref[...])
        w_out_t[...] = jnp.transpose(w_out_ref[...].astype(F32) * 0.5).astype(BF16)
        for k, m in work[:early]:
            slopes(mfrom(k), m)
    with jax.named_scope("x1wait"):
        for k in range(1, msize):
            for m in range(local):
                x1(k, m).wait()

    def pairs(i, carry):
        lanes = pl.ds(pl.multiple_of(i * 128, 128), 128)
        vals = [fcr[q // local, q % local, :, lanes].astype(F32) for q in range(members)]
        total = [jnp.zeros_like(vals[0]) for q in range(members)]
        for a in range(members):
            for b in range(a + 1, members):
                s = slope(vals[a] - vals[b])
                total[a] = total[a] + s
                total[b] = total[b] - s
        goal = tgt[me, :, lanes].astype(F32)
        weight = area[:, lanes]
        for q in range(members):
            d = weight * (slope(vals[q] - goal) - total[q] * (1.0 / members))
            dfs[q // local, q % local, :, lanes] = d.astype(BF16)
        return carry

    tiles = width // 128 // parts
    with jax.named_scope("pairs"):

        def part(p, carry):
            lax.fori_loop(p * tiles, (p + 1) * tiles, pairs, 0)
            for k in range(1, msize):
                lanes = pl.ds(pl.multiple_of(p * share_lanes, 128), share_lanes)
                pltpu.make_async_remote_copy(
                    src_ref=dfs.at[mpeer(k), :, :, lanes],
                    dst_ref=dfr.at[me, :, :, lanes],
                    send_sem=x2s.at[k, p],
                    recv_sem=x2r.at[k, p],
                    device_id=(mpeer(k), sp),
                    device_id_type=MESH,
                ).start()
            return carry

        lax.fori_loop(0, parts, part, 0)
    dfr[me] = dfs[me]
    with jax.named_scope("gap2"):
        for k, m in work[early:]:
            slopes(mfrom(k), m)

    def backward(c, m, rows, inline):
        df = dfr[c, m]
        acc_o[rows, :chans] += lax.dot_general(
            act[c, m, rows, :], df, NT, preferred_element_type=F32
        )
        da = jnp.dot(w_out_t[rows, :], df, preferred_element_type=F32)
        dg = pre[c, m, rows, :]
        if inline:
            dg = gelu_slope(dg)
        dp = (da * dg).astype(BF16)
        act[c, m, rows, :] = dp
        acc_i[rows, :] += jnp.dot(dp, codes(c, m), preferred_element_type=F32)
        dpf = dp.astype(F32)
        tot = dpf[:, :128]
        for i in range(1, width // 128):
            tot = tot + dpf[:, i * 128 : (i + 1) * 128]
        acc_b[rows, :] += tot

    def arrived(k):
        for p in range(parts):
            x2(k, p).wait()

    def bstep(k, carry):
        @pl.when(k > 0)
        def _():
            with jax.named_scope("x2wait"):
                arrived(k)

        with jax.named_scope("bwd"):
            for m in range(local):
                backward(mfrom(k), m, slice(None), False)
        return carry

    lax.fori_loop(0, msize - 2, bstep, 0)

    with jax.named_scope("x2last"):
        arrived(msize - 2)
        arrived(msize - 1)

    todo = [(c, m) for c in range(msize) for m in range(local)]

    def back_to_codes(count):
        for _ in range(min(count, len(todo))):
            c, m = todo.pop(0)
            with jax.named_scope("dlat"):
                d = jnp.dot(w_in_t[...], act[c, m], preferred_element_type=F32)
                code_ref[m, c * width : (c + 1) * width, :] = jnp.transpose(d.astype(BF16))

    def tail_block(j):
        rows = pl.ds(j * BR, BR)
        with jax.named_scope("bwdlast"):
            for m in range(local):
                for k in (msize - 2, msize - 1):
                    backward(mfrom(k), m, rows, k == msize - 1)

    def side_of(j, side):
        rows = pl.ds(pl.multiple_of(j * BR + side * hr, hr), hr)
        bias = jnp.sum(acc_b[rows, :], axis=1, keepdims=True)
        lane = lax.broadcasted_iota(jnp.int32, (hr, 128), 1)
        return acc_i[rows, :], acc_o[rows, :] + jnp.where(lane == chans, bias, 0.0)

    def c1(j):
        return pltpu.make_async_remote_copy(
            src_ref=half.at[j],
            dst_ref=r1.at[j],
            send_sem=p1s.at[j],
            recv_sem=p1r.at[j],
            device_id=(me, partner),
            device_id_type=MESH,
        )

    def c2(j, k):
        return pltpu.make_async_remote_copy(
            src_ref=s2.at[j, mpeer(k)],
            dst_ref=r2.at[j, k],
            send_sem=p2s.at[j, k],
            recv_sem=p2r.at[j, k],
            device_id=(mpeer(k), sp),
            device_id_type=MESH,
        )

    def c3(j, k):
        return pltpu.make_async_remote_copy(
            src_ref=r3.at[j, z],
            dst_ref=r3.at[j, z],
            send_sem=p3s.at[j, k],
            recv_sem=p3r.at[j, k],
            device_id=(me, zpeer(k)),
            device_id_type=MESH,
        )

    def c4(j, k):
        return pltpu.make_async_remote_copy(
            src_ref=full.at[core, j, me],
            dst_ref=full.at[core, j, me],
            send_sem=p4s.at[j, k],
            recv_sem=p4r.at[j, k],
            device_id=(mpeer(k), sp),
            device_id_type=MESH,
        )

    def c5(j, k):
        owner = mfrom(k)
        return pltpu.make_async_remote_copy(
            src_ref=full.at[core, j, owner],
            dst_ref=full.at[core, j, owner],
            send_sem=p5s.at[j, k],
            recv_sem=p5r.at[j, k],
            device_id=(me, partner),
            device_id_type=MESH,
        )

    def stage1(j):
        li, lr = side_of(j, 1 - core)
        half[j, :, :latent] = li.astype(BF16)
        half[j, :, latent:] = lr.astype(BF16)
        c1(j).start()

    def stage2(j):
        mi, mr = side_of(j, core)
        with jax.named_scope(f"w1_{j}"):
            c1(j).wait()
        s2[j, :, :, :latent] = (
            (mi + r1[j, :, :latent].astype(F32)).astype(BF16).reshape(msize, pr, latent)
        )
        s2[j, :, :, latent:] = (
            (mr + r1[j, :, latent:].astype(F32)).astype(BF16).reshape(msize, pr, 128)
        )
        for k in range(1, msize):
            c2(j, k).start()

    def stage3(j):
        with jax.named_scope(f"w2_{j}"):
            for k in range(1, msize):
                c2(j, k).wait()
        summed = s2[j, me].astype(F32)
        for k in range(1, msize):
            summed = summed + r2[j, k].astype(F32)
        r3[j, z] = summed.astype(BF16)
        for k in range(1, zsize):
            c3(j, k).start()

    def stage4(j):
        with jax.named_scope(f"w3_{j}"):
            for k in range(1, zsize):
                c3(j, k).wait()
        summed = r3[j, 0].astype(F32)
        for k in range(1, zsize):
            summed = summed + r3[j, k].astype(F32)
        full[core, j, me] = summed.astype(BF16)
        for k in range(1, msize):
            c4(j, k).start()
        c5(j, 0).start()

    def stage5(j):
        with jax.named_scope(f"w4_{j}"):
            for k in range(1, msize):
                c4(j, k).wait()
                c5(j, k).start()

    scale = 1.0 / math.sqrt(members * cells)

    def stage6(j):
        with jax.named_scope(f"w5_{j}"):
            for k in range(msize):
                c5(j, k).wait()
        for side in range(2):
            lo = j * BR + side * hr
            whole = full[side, j].astype(F32).reshape(hr, latent + 128) * scale
            gwi_ref[lo : lo + hr, :] = whole[:, :latent]
            turned = jnp.transpose(whole[:, latent:])
            gwo_ref[:, lo : lo + hr] = turned[:chans]
            gb_ref[:, lo : lo + hr] = turned[chans : chans + 1]

    for j in range(nb):
        tail_block(j)
        stage1(j)
        if j > 0:
            stage2(j - 1)
    back_to_codes(1)
    stage3(0)
    back_to_codes(1)
    stage2(nb - 1)
    back_to_codes(2)
    stage3(1)
    back_to_codes(2)
    stage3(2)
    back_to_codes(len(todo))
    stage3(3)
    stage4(0)
    stage4(1)
    stage4(2)
    stage5(0)
    stage4(3)
    stage5(1)
    stage6(0)
    stage6(1)
    stage5(2)
    stage5(3)
    stage6(2)
    stage6(3)


def finish(code, gwi, gwo, gb, code_out, gwi_out, gwo_out, gb_out, sems):
    moves = [
        pltpu.make_async_copy(src, dst, sems.at[i])
        for i, (src, dst) in enumerate(
            (
                (code.at[:, pl.ds(0, code_out.shape[1])], code_out),
                (gwi, gwi_out),
                (gwo, gwo_out),
                (gb, gb_out),
            )
        )
    ]
    for move in moves:
        move.start()
    for move in moves:
        move.wait()


def on_device(hidden_codes, w_in, b_in, w_out, b_out, target, band_start):
    local, latent, cells = hidden_codes.shape
    hidden = w_in.shape[0]
    chans = w_out.shape[0]
    msize = lax.axis_size("member")
    ssize = lax.axis_size("space")
    zsize = ssize // 2
    tiles = -(-cells // 128)
    width = -(-tiles // msize) * 128
    nb = hidden // BR
    hr = BR // 2
    pr = hr // msize
    wide = latent + 128
    parts = 2 if (width // 128) % 2 == 0 else 1
    vmem = pl.BlockSpec(memory_space=pltpu.VMEM)
    dma = pltpu.SemaphoreType.DMA
    code, gwi, gwo, gb = pl.pallas_call(
        functools.partial(kernel, msize, ssize, cells),
        out_shape=(
            pltpu.VMEM((local, msize * width, latent), BF16),
            pltpu.VMEM((hidden, latent), F32),
            pltpu.VMEM((chans, hidden), F32),
            pltpu.VMEM((1, hidden), F32),
        ),
        in_specs=[pl.BlockSpec(memory_space=pl.ANY)]
        + [vmem] * 5
        + [pl.BlockSpec(memory_space=pltpu.SMEM)],
        out_specs=(vmem,) * 4,
        scratch_shapes=[
            pltpu.VMEM((msize, chans, width), BF16),
            pltpu.VMEM((1, width), F32),
            pltpu.VMEM((msize, local, hidden, width), BF16),
            pltpu.VMEM((msize, local, hidden, width), F32),
            pltpu.VMEM((msize, local, chans, width), BF16),
            pltpu.VMEM((msize, local, chans, width), BF16),
            pltpu.VMEM((msize, local, chans, width), BF16),
            pltpu.VMEM((hidden, latent), F32),
            pltpu.VMEM((hidden, 128), F32),
            pltpu.VMEM((hidden, 128), F32),
            pltpu.VMEM((nb, hr, wide), BF16),
            pltpu.VMEM((nb, hr, wide), BF16),
            pltpu.VMEM((nb, msize, pr, wide), BF16),
            pltpu.VMEM((nb, msize, pr, wide), BF16),
            pltpu.VMEM((nb, zsize, pr, wide), BF16),
            pltpu.VMEM((2, nb, msize, pr, wide), BF16),
            dma((msize, local)),
            dma((msize, local)),
            dma((msize, parts)),
            dma((msize, parts)),
            dma((nb,)),
            dma((nb,)),
            dma((nb, msize)),
            dma((nb, msize)),
            dma((nb, zsize)),
            dma((nb, zsize)),
            dma((nb, msize)),
            dma((nb, msize)),
            dma((nb, msize)),
            dma((nb, msize)),
            pltpu.VMEM((hidden, latent), BF16),
            pltpu.VMEM((latent, hidden), BF16),
            pltpu.VMEM((hidden, chans), BF16),
            pltpu.VMEM((hidden, 128), F32),
            pltpu.VMEM((chans, 128), F32),
            dma((msize, local)),
        ],
        compiler_params=pltpu.CompilerParams(
            collective_id=0, has_side_effects=True, vmem_limit_bytes=62_000_000
        ),
    )(
        jnp.swapaxes(hidden_codes, 1, 2),
        w_in,
        b_in[None, :],
        w_out,
        b_out[None, :],
        target,
        band_start,
    )
    code, gwi, gwo, gb = pl.pallas_call(
        finish,
        out_shape=(
            jax.ShapeDtypeStruct((local, cells, latent), BF16),
            jax.ShapeDtypeStruct(gwi.shape, F32),
            jax.ShapeDtypeStruct(gwo.shape, F32),
            jax.ShapeDtypeStruct(gb.shape, F32),
        ),
        in_specs=[vmem] * 4,
        out_specs=(pl.BlockSpec(memory_space=pl.ANY),) * 4,
        scratch_shapes=[dma((4,))],
        compiler_params=pltpu.CompilerParams(vmem_limit_bytes=1 << 20),
    )(code, gwi, gwo, gb)
    return jnp.swapaxes(code, 1, 2), gwi, gwo, gb[0]


def solution(mesh):
    in_specs = (P("member", None, "space"), P(), P(), P(), P(), P(None, "space"), P("space"))
    out_specs = (P("member", None, "space"), P(), P(), P())
    return jax.shard_map(
        on_device, mesh=mesh, in_specs=in_specs, out_specs=out_specs, check_vma=False
    )
```

```python
import functools
import math

import jax
import jax.numpy as jnp
from jax import lax
from jax.experimental import pallas as pl
from jax.experimental.pallas import tpu as pltpu
from jax.sharding import PartitionSpec as P

LON = 1440
BR = 256
MESH = pl.DeviceIdType.MESH
NT = (((1,), (1,)), ((), ()))
F32 = jnp.float32
BF16 = jnp.bfloat16
K0 = math.sqrt(2.0 / math.pi)
K1 = K0 * 0.044715


def slope(diff):
    return diff * lax.rsqrt(diff * diff + 0.0625)


def gelu_slope(h):
    q = h * h
    t = jnp.tanh(h * (2.0 * K0 + (8.0 * K1) * q))
    v = (1.0 - t) * (h * (2.0 * K0 + (24.0 * K1) * q))
    return (1.0 + t) * (1.0 + v)


def kernel(
    msize,
    ssize,
    cells,
    hid_ref,
    w_in_ref,
    b_in_ref,
    w_out_ref,
    b_out_ref,
    tgt_ref,
    start_ref,
    code_ref,
    gwi_ref,
    gwo_ref,
    gb_ref,
    tgt,
    area,
    act,
    pre,
    fcs,
    fcr,
    dfr,
    acc_i,
    acc_o,
    acc_b,
    r1,
    s2,
    r2,
    r3,
    full,
    x1s,
    x1r,
    x2s,
    x2r,
    p1s,
    p1r,
    p2s,
    p2r,
    p3s,
    p3r,
    p4s,
    p4r,
    p5s,
    p5r,
    w_half,
    w_in_t,
    w_out_t,
    b_in,
    b_out,
    load,
):
    local = hid_ref.shape[0]
    hidden = w_in_ref.shape[0]
    latent = w_in_ref.shape[1]
    chans = w_out_ref.shape[0]
    width = tgt.shape[1]
    dfs = fcs
    members = local * msize
    zsize = ssize // 2
    ysize = msize // 2
    nb = hidden // BR
    hr = BR // 2
    pr = hr // msize
    parts = x2s.shape[1]
    me = lax.axis_index("member")
    sp = lax.axis_index("space")
    core = lax.rem(sp, 2)
    z = sp // 2
    partner = z * 2 + (1 - core)
    mx = lax.rem(me, 2)
    my = me // 2

    def mpeer(k):
        return lax.rem(my + k // 2, ysize) * 2 + lax.rem(mx + k, 2)

    def mfrom(k):
        return lax.rem(my + ysize - k // 2, ysize) * 2 + lax.rem(mx + k, 2)

    def zpeer(k):
        return lax.rem(z + k, zsize) * 2 + core

    barrier = pltpu.get_barrier_semaphore()
    pl.semaphore_signal(barrier, inc=1, device_id=(me, partner), device_id_type=MESH)
    for k in range(1, msize):
        pl.semaphore_signal(barrier, inc=1, device_id=(mpeer(k), sp), device_id_type=MESH)
    for k in range(1, zsize):
        pl.semaphore_signal(barrier, inc=1, device_id=(me, zpeer(k)), device_id_type=MESH)

    last = msize - 1
    rest = cells - last * width

    def span(c):
        return width if c < last else rest

    def fetch(c, m, n, lo):
        return pltpu.make_async_copy(
            hid_ref.at[m, pl.ds(lo, n)], code_ref.at[m, pl.ds(lo, n)], load.at[c, m]
        )

    def codes(c, m):
        return code_ref[m, pl.ds(pl.multiple_of(c * width, width), width), :]

    for k in range(msize - 1, -1, -1):
        first = mpeer(k)

        @pl.when(first < last)
        def _():
            for m in range(local):
                fetch(first, m, width, pl.multiple_of(first * width, width)).start()

        @pl.when(first == last)
        def _():
            for m in range(local):
                fetch(last, m, rest, last * width).start()

    if rest < width:
        code_ref[:, cells:, :] = jnp.zeros((local, width - rest, latent), BF16)
        tgt[...] = jnp.zeros(tgt.shape, BF16)
    b_in[...] = jnp.transpose(jnp.broadcast_to(b_in_ref[...] * 0.5, (128, hidden)))
    b_out[...] = jnp.transpose(jnp.broadcast_to(b_out_ref[...], (128, chans)))
    w_half[...] = w_in_ref[...] * 0.5

    def x1(k, m):
        return pltpu.make_async_remote_copy(
            src_ref=fcs.at[mpeer(k), m],
            dst_ref=fcr.at[me, m],
            send_sem=x1s.at[k, m],
            recv_sem=x1r.at[k, m],
            device_id=(mpeer(k), sp),
            device_id_type=MESH,
        )

    share_lanes = width // parts

    def x2(k, p):
        lanes = pl.ds(pl.multiple_of(p * share_lanes, 128), share_lanes)
        return pltpu.make_async_remote_copy(
            src_ref=dfs.at[mpeer(k), :, :, lanes],
            dst_ref=dfr.at[me, :, :, lanes],
            send_sem=x2s.at[k, p],
            recv_sem=x2r.at[k, p],
            device_id=(mpeer(k), sp),
            device_id_type=MESH,
        )

    def ready(c):
        for m in range(local):

            @pl.when(c < last)
            def _():
                fetch(c, m, width, 0).wait()

            @pl.when(c == last)
            def _():
                fetch(c, m, rest, 0).wait()

    def forward(c, m):
        x = lax.dot_general(w_half[...], codes(c, m), NT, preferred_element_type=F32)
        h = x + b_in[:, :1]
        pre[c, m] = h
        t = jnp.tanh(h * (2.0 * K0 + (8.0 * K1) * (h * h)))
        act[c, m] = (h + h * t).astype(BF16)
        fc = jnp.dot(w_out_ref[...], act[c, m], preferred_element_type=F32)
        fcs[c, m] = (fc + b_out[:, :1]).astype(BF16)

    def step(i, carry):
        k = last - i
        c = mpeer(k)
        with jax.named_scope("fwd"):
            ready(c)
            for m in range(local):
                forward(c, m)

        @pl.when(i == 0)
        def _():
            pl.semaphore_wait(barrier, msize + zsize - 1)

        @pl.when(k > 0)
        def _():
            for m in range(local):
                x1(k, m).start()

        return carry

    lax.fori_loop(0, msize, step, 0)
    fcr[me] = fcs[me]

    def fold(k, m):
        return m == local - 1 and k < msize - 2 if k < msize - 2 else (k, m) in late

    late = ((msize - 1, local - 1),)

    def slopes(c, m):
        def block(i, carry):
            rows = pl.ds(pl.multiple_of(i * 128, 128), 128)
            pre[c, m, rows, :] = gelu_slope(pre[c, m, rows, :])
            return carry

        lax.fori_loop(0, hidden // 128, block, 0)

    folded = [(k, m) for k in range(msize) for m in range(local) if fold(k, m)]
    work = [(k, m) for k in range(msize) for m in range(local) if (k, m) not in folded]
    early = 2

    with jax.named_scope("gap1"):
        place = me * width + lax.broadcasted_iota(jnp.int32, (1, width), 1)
        row = jnp.zeros((1, width), jnp.int32) + start_ref[0]
        for r in range(1, cells // LON):
            row = row + jnp.where(place >= r * LON, 1, 0)
        angle = (row.astype(F32) + 0.5) * (math.pi / (cells // LON * ssize)) - math.pi / 2
        area[...] = jnp.where(place < cells, jnp.cos(angle), 0.0)
        acc_i[...] = jnp.zeros_like(acc_i)
        acc_o[...] = jnp.zeros_like(acc_o)
        acc_b[...] = jnp.zeros_like(acc_b)
        for c in range(msize):

            @pl.when(me == c)
            def _():
                n = span(c)
                tgt[:, :n] = tgt_ref[:, c * width : c * width + n]
        w_in_t[...] = jnp.transpose(w_in_ref[...])
        w_out_t[...] = jnp.transpose(w_out_ref[...].astype(F32) * 0.5).astype(BF16)
        for k, m in work[:early]:
            slopes(mfrom(k), m)
    with jax.named_scope("x1wait"):
        for k in range(1, msize):
            for m in range(local):
                x1(k, m).wait()

    def pairs(i, carry):
        lanes = pl.ds(pl.multiple_of(i * 128, 128), 128)
        vals = [fcr[q // local, q % local, :, lanes].astype(F32) for q in range(members)]
        total = [jnp.zeros_like(vals[0]) for q in range(members)]
        for a in range(members):
            for b in range(a + 1, members):
                s = slope(vals[a] - vals[b])
                total[a] = total[a] + s
                total[b] = total[b] - s
        goal = tgt[:, lanes].astype(F32)
        weight = area[:, lanes]
        for q in range(members):
            d = weight * (slope(vals[q] - goal) - total[q] * (1.0 / members))
            dfs[q // local, q % local, :, lanes] = d.astype(BF16)
        return carry

    tiles = width // 128 // parts
    with jax.named_scope("pairs"):

        def part(p, carry):
            lax.fori_loop(p * tiles, (p + 1) * tiles, pairs, 0)
            for k in range(1, last):
                x2(k, p).start()
            return carry

        lax.fori_loop(0, parts, part, 0)
        for p in range(parts):
            x2(last, p).start()
    dfr[me] = dfs[me]
    with jax.named_scope("gap2"):
        for k, m in work[early:]:
            slopes(mfrom(k), m)

    def backward(c, m, rows, inner, inline):
        df = dfr[c, m]
        if inner:
            outer = lax.dot_general(df, act[c, m, rows, :], NT, preferred_element_type=F32)
        else:
            outer = jnp.dot(df, jnp.transpose(act[c, m, rows, :]), preferred_element_type=F32)
        acc_o[:chans, rows] += outer
        da = jnp.dot(w_out_t[rows, :], df, preferred_element_type=F32)
        dg = pre[c, m, rows, :]
        if inline:
            dg = gelu_slope(dg)
        dp = (da * dg).astype(BF16)
        act[c, m, rows, :] = dp
        acc_i[rows, :] += jnp.dot(dp, codes(c, m), preferred_element_type=F32)
        dpf = dp.astype(F32)
        tot = dpf[:, :128]
        for i in range(1, width // 128):
            tot = tot + dpf[:, i * 128 : (i + 1) * 128]
        acc_b[rows, :] += tot

    def arrived(k):
        for p in range(parts):
            x2(k, p).wait()

    def bstep(k, carry):
        @pl.when(k > 0)
        def _():
            with jax.named_scope("x2wait"):
                arrived(k)

        with jax.named_scope("bwd"):
            for m in range(local):
                backward(mfrom(k), m, slice(None), False, m == local - 1)
        return carry

    lax.fori_loop(0, msize - 2, bstep, 0)

    with jax.named_scope("x2last"):
        arrived(msize - 2)
        arrived(msize - 1)

    todo = [(c, m) for c in range(msize) for m in range(local)]

    def back_to_codes(count):
        for _ in range(min(count, len(todo))):
            c, m = todo.pop(0)
            with jax.named_scope("dlat"):
                d = jnp.dot(w_in_t[...], act[c, m], preferred_element_type=F32)
                code_ref[m, c * width : (c + 1) * width, :] = jnp.transpose(d.astype(BF16))

    def tail_block(j, k):
        rows = pl.ds(pl.multiple_of(j * BR, BR), BR)
        with jax.named_scope("bwdlast"):
            for m in range(local):
                backward(mfrom(k), m, rows, True, fold(k, m))

    def side_of(j, side):
        rows = pl.ds(pl.multiple_of(j * BR + side * hr, hr), hr)
        bias = jnp.sum(acc_b[rows, :], axis=1, keepdims=True)
        lane = lax.broadcasted_iota(jnp.int32, (hr, 128), 1)
        return acc_i[rows, :], jnp.transpose(acc_o[:, rows]) + jnp.where(lane == chans, bias, 0.0)

    def c1(j):
        return pltpu.make_async_remote_copy(
            src_ref=s2.at[j],
            dst_ref=r1.at[j],
            send_sem=p1s.at[j],
            recv_sem=p1r.at[j],
            device_id=(me, partner),
            device_id_type=MESH,
        )

    def c2(j, k):
        return pltpu.make_async_remote_copy(
            src_ref=s2.at[j, mpeer(k)],
            dst_ref=r2.at[j, k],
            send_sem=p2s.at[j, k],
            recv_sem=p2r.at[j, k],
            device_id=(mpeer(k), sp),
            device_id_type=MESH,
        )

    def c3(j, k):
        return pltpu.make_async_remote_copy(
            src_ref=r3.at[j, z],
            dst_ref=r3.at[j, z],
            send_sem=p3s.at[j, k],
            recv_sem=p3r.at[j, k],
            device_id=(me, zpeer(k)),
            device_id_type=MESH,
        )

    def c4(j, k):
        return pltpu.make_async_remote_copy(
            src_ref=full.at[core, j, me],
            dst_ref=full.at[core, j, me],
            send_sem=p4s.at[j, k],
            recv_sem=p4r.at[j, k],
            device_id=(mpeer(k), sp),
            device_id_type=MESH,
        )

    def c5(j, k):
        owner = mfrom(k)
        return pltpu.make_async_remote_copy(
            src_ref=full.at[core, j, owner],
            dst_ref=full.at[core, j, owner],
            send_sem=p5s.at[j, k],
            recv_sem=p5r.at[j, k],
            device_id=(me, partner),
            device_id_type=MESH,
        )

    def stage1(j):
        li, lr = side_of(j, 1 - core)
        s2[j, :, :, :latent] = li.astype(BF16).reshape(msize, pr, latent)
        s2[j, :, :, latent:] = lr.astype(BF16).reshape(msize, pr, 128)
        c1(j).start()

    def stage2(j):
        mi, mr = side_of(j, core)
        c1(j).wait()
        s2[j, :, :, :latent] = (
            (mi.reshape(msize, pr, latent) + r1[j, :, :, :latent].astype(F32)).astype(BF16)
        )
        s2[j, :, :, latent:] = (
            (mr.reshape(msize, pr, 128) + r1[j, :, :, latent:].astype(F32)).astype(BF16)
        )
        for k in range(1, msize):
            c2(j, k).start()

    def stage3(j):
        with jax.named_scope(f"w2_{j}"):
            for k in range(1, msize):
                c2(j, k).wait()
        summed = s2[j, me].astype(F32)
        for k in range(1, msize):
            summed = summed + r2[j, k].astype(F32)
        r3[j, z] = summed.astype(BF16)
        for k in range(1, zsize):
            c3(j, k).start()

    def stage4(j):
        with jax.named_scope(f"w3_{j}"):
            for k in range(1, zsize):
                c3(j, k).wait()
        summed = r3[j, 0].astype(F32)
        for k in range(1, zsize):
            summed = summed + r3[j, k].astype(F32)
        full[core, j, me] = summed.astype(BF16)
        for k in range(1, msize):
            c4(j, k).start()
        c5(j, 0).start()

    def stage5(j):
        with jax.named_scope(f"w4_{j}"):
            for k in range(1, msize):
                c4(j, k).wait()
                c5(j, k).start()

    scale = 1.0 / math.sqrt(members * cells)

    def stage6(j):
        with jax.named_scope(f"w5_{j}"):
            for k in range(msize):
                c5(j, k).wait()
        for side in range(2):
            lo = j * BR + side * hr
            whole = full[side, j].astype(F32).reshape(hr, latent + 128) * scale
            gwi_ref[lo : lo + hr, :] = whole[:, :latent]
            turned = jnp.transpose(whole[:, latent:])
            gwo_ref[:, lo : lo + hr] = turned[:chans]
            gb_ref[:, lo : lo + hr] = turned[chans : chans + 1]

    def tstep(j, carry):
        tail_block(j, msize - 2)
        tail_block(j, msize - 1)

        @pl.when(j > 0)
        def _():
            stage2(j - 1)

        stage1(j)
        return carry

    lax.fori_loop(0, nb, tstep, 0)
    stage3(0)
    back_to_codes(2)
    stage2(nb - 1)
    stage3(1)
    back_to_codes(3)
    stage3(2)
    back_to_codes(len(todo))
    stage3(3)
    stage4(0)
    stage4(1)
    stage4(2)
    stage5(0)
    stage4(3)
    stage5(1)
    stage6(0)
    stage6(1)
    stage5(2)
    stage5(3)
    stage6(2)
    stage6(3)


def finish(code, gwi, gwo, gb, code_out, gwi_out, gwo_out, gb_out, sems):
    moves = [
        pltpu.make_async_copy(src, dst, sems.at[i])
        for i, (src, dst) in enumerate(
            (
                (code.at[:, pl.ds(0, code_out.shape[1])], code_out),
                (gwi, gwi_out),
                (gwo, gwo_out),
                (gb, gb_out),
            )
        )
    ]
    for move in moves:
        move.start()
    for move in moves:
        move.wait()


def on_device(hidden_codes, w_in, b_in, w_out, b_out, target, band_start):
    local, latent, cells = hidden_codes.shape
    hidden = w_in.shape[0]
    chans = w_out.shape[0]
    msize = lax.axis_size("member")
    ssize = lax.axis_size("space")
    zsize = ssize // 2
    tiles = -(-cells // 128)
    width = -(-tiles // msize) * 128
    nb = hidden // BR
    hr = BR // 2
    pr = hr // msize
    wide = latent + 128
    parts = 2 if (width // 128) % 2 == 0 else 1
    vmem = pl.BlockSpec(memory_space=pltpu.VMEM)
    dma = pltpu.SemaphoreType.DMA
    code, gwi, gwo, gb = pl.pallas_call(
        functools.partial(kernel, msize, ssize, cells),
        out_shape=(
            pltpu.VMEM((local, msize * width, latent), BF16),
            pltpu.VMEM((hidden, latent), F32),
            pltpu.VMEM((chans, hidden), F32),
            pltpu.VMEM((1, hidden), F32),
        ),
        in_specs=[pl.BlockSpec(memory_space=pl.ANY)]
        + [vmem] * 5
        + [pl.BlockSpec(memory_space=pltpu.SMEM)],
        out_specs=(vmem,) * 4,
        scratch_shapes=[
            pltpu.VMEM((chans, width), BF16),
            pltpu.VMEM((1, width), F32),
            pltpu.VMEM((msize, local, hidden, width), BF16),
            pltpu.VMEM((msize, local, hidden, width), F32),
            pltpu.VMEM((msize, local, chans, width), BF16),
            pltpu.VMEM((msize, local, chans, width), BF16),
            pltpu.VMEM((msize, local, chans, width), BF16),
            pltpu.VMEM((hidden, latent), F32),
            pltpu.VMEM((128, hidden), F32),
            pltpu.VMEM((hidden, 128), F32),
            pltpu.VMEM((nb, msize, pr, wide), BF16),
            pltpu.VMEM((nb, msize, pr, wide), BF16),
            pltpu.VMEM((nb, msize, pr, wide), BF16),
            pltpu.VMEM((nb, zsize, pr, wide), BF16),
            pltpu.VMEM((2, nb, msize, pr, wide), BF16),
            dma((msize, local)),
            dma((msize, local)),
            dma((msize, parts)),
            dma((msize, parts)),
            dma((nb,)),
            dma((nb,)),
            dma((nb, msize)),
            dma((nb, msize)),
            dma((nb, zsize)),
            dma((nb, zsize)),
            dma((nb, msize)),
            dma((nb, msize)),
            dma((nb, msize)),
            dma((nb, msize)),
            pltpu.VMEM((hidden, latent), BF16),
            pltpu.VMEM((latent, hidden), BF16),
            pltpu.VMEM((hidden, chans), BF16),
            pltpu.VMEM((hidden, 128), F32),
            pltpu.VMEM((chans, 128), F32),
            dma((msize, local)),
        ],
        compiler_params=pltpu.CompilerParams(
            collective_id=0, has_side_effects=True, vmem_limit_bytes=62_000_000
        ),
    )(
        jnp.swapaxes(hidden_codes, 1, 2),
        w_in,
        b_in[None, :],
        w_out,
        b_out[None, :],
        target,
        band_start,
    )
    code, gwi, gwo, gb = pl.pallas_call(
        finish,
        out_shape=(
            jax.ShapeDtypeStruct((local, cells, latent), BF16),
            jax.ShapeDtypeStruct(gwi.shape, F32),
            jax.ShapeDtypeStruct(gwo.shape, F32),
            jax.ShapeDtypeStruct(gb.shape, F32),
        ),
        in_specs=[vmem] * 4,
        out_specs=(pl.BlockSpec(memory_space=pl.ANY),) * 4,
        scratch_shapes=[dma((4,))],
        compiler_params=pltpu.CompilerParams(vmem_limit_bytes=1 << 20),
    )(code, gwi, gwo, gb)
    return jnp.swapaxes(code, 1, 2), gwi, gwo, gb[0]


def solution(mesh):
    in_specs = (P("member", None, "space"), P(), P(), P(), P(), P(None, "space"), P("space"))
    out_specs = (P("member", None, "space"), P(), P(), P())
    return jax.shard_map(
        on_device, mesh=mesh, in_specs=in_specs, out_specs=out_specs, check_vma=False
    )
```

```python
import functools
import math

import jax
import jax.numpy as jnp
from jax import lax
from jax.experimental import pallas as pl
from jax.experimental.pallas import tpu as pltpu
from jax.sharding import PartitionSpec as P

LON = 1440
BR = 256
MESH = pl.DeviceIdType.MESH
NT = (((1,), (1,)), ((), ()))
F32 = jnp.float32
BF16 = jnp.bfloat16
K0 = math.sqrt(2.0 / math.pi)
K1 = K0 * 0.044715


def slope(diff):
    return diff * lax.rsqrt(diff * diff + 0.0625)


def gelu_slope(h):
    q = h * h
    t = jnp.tanh(h * (2.0 * K0 + (8.0 * K1) * q))
    v = (1.0 - t) * (h * (2.0 * K0 + (24.0 * K1) * q))
    return (1.0 + t) * (1.0 + v)


def kernel(
    msize,
    ssize,
    cells,
    hid_ref,
    w_in_ref,
    b_in_ref,
    w_out_ref,
    b_out_ref,
    tgt_ref,
    start_ref,
    code_ref,
    gwi_ref,
    gwo_ref,
    gb_ref,
    tgt,
    area,
    act,
    pre,
    fcs,
    fcr,
    dfr,
    acc_i,
    acc_o,
    acc_b,
    r1,
    s2,
    r2,
    r3,
    full,
    x1s,
    x1r,
    x2s,
    x2r,
    p1s,
    p1r,
    p2s,
    p2r,
    p3s,
    p3r,
    p4s,
    p4r,
    p5s,
    p5r,
    w_half,
    w_in_t,
    w_out_t,
    b_in,
    b_out,
    load,
):
    local = hid_ref.shape[0]
    hidden = w_in_ref.shape[0]
    latent = w_in_ref.shape[1]
    chans = w_out_ref.shape[0]
    width = tgt.shape[1]
    dfs = fcs
    members = local * msize
    zsize = ssize // 2
    ysize = msize // 2
    nb = hidden // BR
    hr = BR // 2
    pr = hr // msize
    parts = x2s.shape[1]
    me = lax.axis_index("member")
    sp = lax.axis_index("space")
    core = lax.rem(sp, 2)
    z = sp // 2
    partner = z * 2 + (1 - core)
    mx = lax.rem(me, 2)
    my = me // 2

    def mpeer(k):
        return lax.rem(my + k // 2, ysize) * 2 + lax.rem(mx + k, 2)

    def mfrom(k):
        return lax.rem(my + ysize - k // 2, ysize) * 2 + lax.rem(mx + k, 2)

    def zpeer(k):
        return lax.rem(z + k, zsize) * 2 + core

    barrier = pltpu.get_barrier_semaphore()
    pl.semaphore_signal(barrier, inc=1, device_id=(me, partner), device_id_type=MESH)
    for k in range(1, msize):
        pl.semaphore_signal(barrier, inc=1, device_id=(mpeer(k), sp), device_id_type=MESH)
    for k in range(1, zsize):
        pl.semaphore_signal(barrier, inc=1, device_id=(me, zpeer(k)), device_id_type=MESH)

    last = msize - 1
    rest = cells - last * width

    def span(c):
        return width if c < last else rest

    def fetch(c, m, n, lo):
        return pltpu.make_async_copy(
            hid_ref.at[m, pl.ds(lo, n)], code_ref.at[m, pl.ds(lo, n)], load.at[c, m]
        )

    def codes(c, m):
        return code_ref[m, pl.ds(pl.multiple_of(c * width, width), width), :]

    for k in range(msize - 1, -1, -1):
        first = mpeer(k)

        @pl.when(first < last)
        def _():
            for m in range(local):
                fetch(first, m, width, pl.multiple_of(first * width, width)).start()

        @pl.when(first == last)
        def _():
            for m in range(local):
                fetch(last, m, rest, last * width).start()

    if rest < width:
        code_ref[:, cells:, :] = jnp.zeros((local, width - rest, latent), BF16)
        tgt[...] = jnp.zeros(tgt.shape, BF16)
    b_in[...] = jnp.transpose(jnp.broadcast_to(b_in_ref[...] * 0.5, (128, hidden)))
    b_out[...] = jnp.transpose(jnp.broadcast_to(b_out_ref[...], (128, chans)))
    w_half[...] = w_in_ref[...] * 0.5

    def x1(k, m):
        return pltpu.make_async_remote_copy(
            src_ref=fcs.at[mpeer(k), m],
            dst_ref=fcr.at[me, m],
            send_sem=x1s.at[k, m],
            recv_sem=x1r.at[k, m],
            device_id=(mpeer(k), sp),
            device_id_type=MESH,
        )

    share_lanes = width // parts

    def x2(k, p):
        lanes = pl.ds(pl.multiple_of(p * share_lanes, 128), share_lanes)
        return pltpu.make_async_remote_copy(
            src_ref=dfs.at[mpeer(k), :, :, lanes],
            dst_ref=dfr.at[me, :, :, lanes],
            send_sem=x2s.at[k, p],
            recv_sem=x2r.at[k, p],
            device_id=(mpeer(k), sp),
            device_id_type=MESH,
        )

    def ready(c):
        for m in range(local):

            @pl.when(c < last)
            def _():
                fetch(c, m, width, 0).wait()

            @pl.when(c == last)
            def _():
                fetch(c, m, rest, 0).wait()

    def forward(c, m):
        x = lax.dot_general(w_half[...], codes(c, m), NT, preferred_element_type=F32)
        h = x + b_in[:, :1]
        pre[c, m] = h
        t = jnp.tanh(h * (2.0 * K0 + (8.0 * K1) * (h * h)))
        act[c, m] = (h + h * t).astype(BF16)
        fc = jnp.dot(w_out_ref[...], act[c, m], preferred_element_type=F32)
        fcs[c, m] = (fc + b_out[:, :1]).astype(BF16)

    def step(i, carry):
        k = last - i
        c = mpeer(k)
        with jax.named_scope("fwd"):
            ready(c)
            for m in range(local):
                forward(c, m)

        @pl.when(i == 0)
        def _():
            pl.semaphore_wait(barrier, msize + zsize - 1)

        @pl.when(k > 0)
        def _():
            for m in range(local):
                x1(k, m).start()

        return carry

    lax.fori_loop(0, msize, step, 0)
    fcr[me] = fcs[me]

    def fold(k, m):
        return m == local - 1 and k < msize - 2 if k < msize - 2 else (k, m) in late

    late = ((msize - 1, local - 1),)

    def slopes(c, m):
        def block(i, carry):
            rows = pl.ds(pl.multiple_of(i * 128, 128), 128)
            pre[c, m, rows, :] = gelu_slope(pre[c, m, rows, :])
            return carry

        lax.fori_loop(0, hidden // 128, block, 0)

    folded = [(k, m) for k in range(msize) for m in range(local) if fold(k, m)]
    work = [(k, m) for k in range(msize) for m in range(local) if (k, m) not in folded]
    early = 3

    with jax.named_scope("gap1"):
        place = me * width + lax.broadcasted_iota(jnp.int32, (1, width), 1)
        row = jnp.zeros((1, width), jnp.int32) + start_ref[0]
        for r in range(1, cells // LON):
            row = row + jnp.where(place >= r * LON, 1, 0)
        angle = (row.astype(F32) + 0.5) * (math.pi / (cells // LON * ssize)) - math.pi / 2
        area[...] = jnp.where(place < cells, jnp.cos(angle), 0.0)
        acc_i[...] = jnp.zeros_like(acc_i)
        acc_o[...] = jnp.zeros_like(acc_o)
        acc_b[...] = jnp.zeros_like(acc_b)
        for c in range(msize):

            @pl.when(me == c)
            def _():
                n = span(c)
                tgt[:, :n] = tgt_ref[:, c * width : c * width + n]
        w_in_t[...] = jnp.transpose(w_in_ref[...])
        w_out_t[...] = jnp.transpose(w_out_ref[...].astype(F32) * 0.5).astype(BF16)
        for k, m in work[:early]:
            slopes(mfrom(k), m)
    with jax.named_scope("x1wait"):
        for k in range(1, msize):
            for m in range(local):
                x1(k, m).wait()

    def pairs(i, carry):
        lanes = pl.ds(pl.multiple_of(i * 128, 128), 128)
        vals = [fcr[q // local, q % local, :, lanes].astype(F32) for q in range(members)]
        total = [jnp.zeros_like(vals[0]) for q in range(members)]
        for a in range(members):
            for b in range(a + 1, members):
                s = slope(vals[a] - vals[b])
                total[a] = total[a] + s
                total[b] = total[b] - s
        goal = tgt[:, lanes].astype(F32)
        weight = area[:, lanes]
        for q in range(members):
            d = weight * (slope(vals[q] - goal) - total[q] * (1.0 / members))
            dfs[q // local, q % local, :, lanes] = d.astype(BF16)
        return carry

    tiles = width // 128 // parts
    with jax.named_scope("pairs"):

        def part(p, carry):
            lax.fori_loop(p * tiles, (p + 1) * tiles, pairs, 0)
            for k in range(1, last):
                x2(k, p).start()
            return carry

        lax.fori_loop(0, parts, part, 0)
        for p in range(parts):
            x2(last, p).start()
    dfr[me] = dfs[me]
    with jax.named_scope("gap2"):
        for k, m in work[early:]:
            slopes(mfrom(k), m)

    def backward(c, m, rows, inner, inline):
        df = dfr[c, m]
        if inner:
            outer = lax.dot_general(df, act[c, m, rows, :], NT, preferred_element_type=F32)
        else:
            outer = jnp.dot(df, jnp.transpose(act[c, m, rows, :]), preferred_element_type=F32)
        acc_o[:chans, rows] += outer
        da = jnp.dot(w_out_t[rows, :], df, preferred_element_type=F32)
        dg = pre[c, m, rows, :]
        if inline:
            dg = gelu_slope(dg)
        dp = (da * dg).astype(BF16)
        act[c, m, rows, :] = dp
        acc_i[rows, :] += jnp.dot(dp, codes(c, m), preferred_element_type=F32)
        dpf = dp.astype(F32)
        tot = dpf[:, :128]
        for i in range(1, width // 128):
            tot = tot + dpf[:, i * 128 : (i + 1) * 128]
        acc_b[rows, :] += tot

    def arrived(k):
        for p in range(parts):
            x2(k, p).wait()

    def bstep(k, carry):
        @pl.when(k > 0)
        def _():
            with jax.named_scope("x2wait"):
                arrived(k)

        with jax.named_scope("bwd"):
            for m in range(local):
                backward(mfrom(k), m, slice(None), False, m == local - 1)
        return carry

    lax.fori_loop(0, msize - 2, bstep, 0)

    with jax.named_scope("x2last"):
        arrived(msize - 2)
        arrived(msize - 1)

    todo = [(c, m) for c in range(msize) for m in range(local)]

    def back_to_codes(count):
        for _ in range(min(count, len(todo))):
            c, m = todo.pop(0)
            with jax.named_scope("dlat"):
                d = jnp.dot(w_in_t[...], act[c, m], preferred_element_type=F32)
                code_ref[m, c * width : (c + 1) * width, :] = jnp.transpose(d.astype(BF16))

    def tail_block(j, k):
        rows = pl.ds(pl.multiple_of(j * BR, BR), BR)
        with jax.named_scope("bwdlast"):
            for m in range(local):
                backward(mfrom(k), m, rows, True, fold(k, m))

    def side_of(j, side):
        rows = pl.ds(pl.multiple_of(j * BR + side * hr, hr), hr)
        bias = jnp.sum(acc_b[rows, :], axis=1, keepdims=True)
        lane = lax.broadcasted_iota(jnp.int32, (hr, 128), 1)
        return acc_i[rows, :], jnp.transpose(acc_o[:, rows]) + jnp.where(lane == chans, bias, 0.0)

    def c1(j):
        return pltpu.make_async_remote_copy(
            src_ref=s2.at[j],
            dst_ref=r1.at[j],
            send_sem=p1s.at[j],
            recv_sem=p1r.at[j],
            device_id=(me, partner),
            device_id_type=MESH,
        )

    def c2(j, k):
        return pltpu.make_async_remote_copy(
            src_ref=s2.at[j, mpeer(k)],
            dst_ref=r2.at[j, k],
            send_sem=p2s.at[j, k],
            recv_sem=p2r.at[j, k],
            device_id=(mpeer(k), sp),
            device_id_type=MESH,
        )

    def c3(j, k):
        return pltpu.make_async_remote_copy(
            src_ref=r3.at[j, z],
            dst_ref=r3.at[j, z],
            send_sem=p3s.at[j, k],
            recv_sem=p3r.at[j, k],
            device_id=(me, zpeer(k)),
            device_id_type=MESH,
        )

    def c4(j, k):
        return pltpu.make_async_remote_copy(
            src_ref=full.at[core, j, me],
            dst_ref=full.at[core, j, me],
            send_sem=p4s.at[j, k],
            recv_sem=p4r.at[j, k],
            device_id=(mpeer(k), sp),
            device_id_type=MESH,
        )

    def c5(j, k):
        owner = mfrom(k)
        return pltpu.make_async_remote_copy(
            src_ref=full.at[core, j, owner],
            dst_ref=full.at[core, j, owner],
            send_sem=p5s.at[j, k],
            recv_sem=p5r.at[j, k],
            device_id=(me, partner),
            device_id_type=MESH,
        )

    def stage1(j):
        li, lr = side_of(j, 1 - core)
        s2[j, :, :, :latent] = li.astype(BF16).reshape(msize, pr, latent)
        s2[j, :, :, latent:] = lr.astype(BF16).reshape(msize, pr, 128)
        c1(j).start()

    def stage2(j):
        mi, mr = side_of(j, core)
        c1(j).wait()
        s2[j, :, :, :latent] = (
            (mi.reshape(msize, pr, latent) + r1[j, :, :, :latent].astype(F32)).astype(BF16)
        )
        s2[j, :, :, latent:] = (
            (mr.reshape(msize, pr, 128) + r1[j, :, :, latent:].astype(F32)).astype(BF16)
        )
        for k in range(1, msize):
            c2(j, k).start()

    def stage3(j):
        with jax.named_scope(f"w2_{j}"):
            for k in range(1, msize):
                c2(j, k).wait()
        summed = s2[j, me].astype(F32)
        for k in range(1, msize):
            summed = summed + r2[j, k].astype(F32)
        r3[j, z] = summed.astype(BF16)
        for k in range(1, zsize):
            c3(j, k).start()

    def stage4(j):
        with jax.named_scope(f"w3_{j}"):
            for k in range(1, zsize):
                c3(j, k).wait()
        summed = r3[j, 0].astype(F32)
        for k in range(1, zsize):
            summed = summed + r3[j, k].astype(F32)
        full[core, j, me] = summed.astype(BF16)
        for k in range(1, msize):
            c4(j, k).start()
        c5(j, 0).start()

    def stage5(j):
        with jax.named_scope(f"w4_{j}"):
            for k in range(1, msize):
                c4(j, k).wait()
                c5(j, k).start()

    scale = 1.0 / math.sqrt(members * cells)

    def stage6(j):
        with jax.named_scope(f"w5_{j}"):
            for k in range(msize):
                c5(j, k).wait()
        for side in range(2):
            lo = j * BR + side * hr
            whole = full[side, j].astype(F32).reshape(hr, latent + 128) * scale
            gwi_ref[lo : lo + hr, :] = whole[:, :latent]
            turned = jnp.transpose(whole[:, latent:])
            gwo_ref[:, lo : lo + hr] = turned[:chans]
            gb_ref[:, lo : lo + hr] = turned[chans : chans + 1]

    def tstep(j, carry):
        tail_block(j, msize - 2)
        tail_block(j, msize - 1)

        @pl.when(j > 0)
        def _():
            stage2(j - 1)

        stage1(j)
        return carry

    lax.fori_loop(0, nb, tstep, 0)
    stage3(0)
    back_to_codes(2)
    stage2(nb - 1)
    stage3(1)
    back_to_codes(3)
    stage3(2)
    back_to_codes(2)
    stage3(3)
    back_to_codes(len(todo))
    stage4(0)
    stage4(1)
    stage4(2)
    stage5(0)
    stage4(3)
    stage5(1)
    stage6(0)
    stage6(1)
    stage5(2)
    stage5(3)
    stage6(2)
    stage6(3)


def finish(code, gwi, gwo, gb, code_out, gwi_out, gwo_out, gb_out, sems):
    moves = [
        pltpu.make_async_copy(src, dst, sems.at[i])
        for i, (src, dst) in enumerate(
            (
                (code.at[:, pl.ds(0, code_out.shape[1])], code_out),
                (gwi, gwi_out),
                (gwo, gwo_out),
                (gb, gb_out),
            )
        )
    ]
    for move in moves:
        move.start()
    for move in moves:
        move.wait()


def on_device(hidden_codes, w_in, b_in, w_out, b_out, target, band_start):
    local, latent, cells = hidden_codes.shape
    hidden = w_in.shape[0]
    chans = w_out.shape[0]
    msize = lax.axis_size("member")
    ssize = lax.axis_size("space")
    zsize = ssize // 2
    tiles = -(-cells // 128)
    width = -(-tiles // msize) * 128
    nb = hidden // BR
    hr = BR // 2
    pr = hr // msize
    wide = latent + 128
    parts = 2 if (width // 128) % 2 == 0 else 1
    vmem = pl.BlockSpec(memory_space=pltpu.VMEM)
    dma = pltpu.SemaphoreType.DMA
    code, gwi, gwo, gb = pl.pallas_call(
        functools.partial(kernel, msize, ssize, cells),
        out_shape=(
            pltpu.VMEM((local, msize * width, latent), BF16),
            pltpu.VMEM((hidden, latent), F32),
            pltpu.VMEM((chans, hidden), F32),
            pltpu.VMEM((1, hidden), F32),
        ),
        in_specs=[pl.BlockSpec(memory_space=pl.ANY)]
        + [vmem] * 5
        + [pl.BlockSpec(memory_space=pltpu.SMEM)],
        out_specs=(vmem,) * 4,
        scratch_shapes=[
            pltpu.VMEM((chans, width), BF16),
            pltpu.VMEM((1, width), F32),
            pltpu.VMEM((msize, local, hidden, width), BF16),
            pltpu.VMEM((msize, local, hidden, width), F32),
            pltpu.VMEM((msize, local, chans, width), BF16),
            pltpu.VMEM((msize, local, chans, width), BF16),
            pltpu.VMEM((msize, local, chans, width), BF16),
            pltpu.VMEM((hidden, latent), F32),
            pltpu.VMEM((128, hidden), F32),
            pltpu.VMEM((hidden, 128), F32),
            pltpu.VMEM((nb, msize, pr, wide), BF16),
            pltpu.VMEM((nb, msize, pr, wide), BF16),
            pltpu.VMEM((nb, msize, pr, wide), BF16),
            pltpu.VMEM((nb, zsize, pr, wide), BF16),
            pltpu.VMEM((2, nb, msize, pr, wide), BF16),
            dma((msize, local)),
            dma((msize, local)),
            dma((msize, parts)),
            dma((msize, parts)),
            dma((nb,)),
            dma((nb,)),
            dma((nb, msize)),
            dma((nb, msize)),
            dma((nb, zsize)),
            dma((nb, zsize)),
            dma((nb, msize)),
            dma((nb, msize)),
            dma((nb, msize)),
            dma((nb, msize)),
            pltpu.VMEM((hidden, latent), BF16),
            pltpu.VMEM((latent, hidden), BF16),
            pltpu.VMEM((hidden, chans), BF16),
            pltpu.VMEM((hidden, 128), F32),
            pltpu.VMEM((chans, 128), F32),
            dma((msize, local)),
        ],
        compiler_params=pltpu.CompilerParams(
            collective_id=0, has_side_effects=True, vmem_limit_bytes=62_000_000
        ),
    )(
        jnp.swapaxes(hidden_codes, 1, 2),
        w_in,
        b_in[None, :],
        w_out,
        b_out[None, :],
        target,
        band_start,
    )
    code, gwi, gwo, gb = pl.pallas_call(
        finish,
        out_shape=(
            jax.ShapeDtypeStruct((local, cells, latent), BF16),
            jax.ShapeDtypeStruct(gwi.shape, F32),
            jax.ShapeDtypeStruct(gwo.shape, F32),
            jax.ShapeDtypeStruct(gb.shape, F32),
        ),
        in_specs=[vmem] * 4,
        out_specs=(pl.BlockSpec(memory_space=pl.ANY),) * 4,
        scratch_shapes=[dma((4,))],
        compiler_params=pltpu.CompilerParams(vmem_limit_bytes=1 << 20),
    )(code, gwi, gwo, gb)
    return jnp.swapaxes(code, 1, 2), gwi, gwo, gb[0]


def solution(mesh):
    in_specs = (P("member", None, "space"), P(), P(), P(), P(), P(None, "space"), P("space"))
    out_specs = (P("member", None, "space"), P(), P(), P())
    return jax.shard_map(
        on_device, mesh=mesh, in_specs=in_specs, out_specs=out_specs, check_vma=False
    )
```
